128 devices in a mesh: curve: 8 (over x, core), group: 16 (over y, z).
Axes of the slice: x: 4, y: 4, z: 4, core: 2. Of those that a mesh axis runs over, the one named last changes fastest.
Arguments:
- composition: float32 [6144, 53, 256], P(('curve', 'group')), may hold values from -4 to 4
- heat_level: float32 [6144, 256], P(('curve', 'group')), may hold values from 1000 to 2500
- step_counts: int32 [6144], P(('curve', 'group')), may hold values from 1 to 3
- burning_parcel_roster: int32 [768], P(('curve', 'group')), may hold values from 0 to 47, as said below
- target_compute_place: int32 [768], P(('curve', 'group')), may hold values from -1 to 383, as said below
- partial_reciprocal_operator: float32 [768, 53, 53], P(('curve', 'group')), may hold values from -0.03 to 0.13
- speed_log_prefactor: float32 [268], replicated, may hold values from -1 to 1
- arrhenius_barrier: float32 [268], replicated, may hold values from 0.5 to 4
- leading_ingredient: float32 [268, 53], replicated, may hold values from -0.875 to 0.875
- trailing_ingredient: float32 [268, 53], replicated, may hold values from -0.875 to 0.875
- molar_coefficients: float32 [53, 268], replicated, may hold values from -0.375 to 0.375
Outputs:
- new_species: float32 [6144, 53, 256], P(('curve', 'group'))
The draws below stay inside these ranges and needn't reach their ends.
Inputs may be any that keep to these rules, and one draw needn't show every extreme that they name: `burning_parcel_roster`: each owner's 6 entries name distinct blocks among its own 48 blocks. `target_compute_place`: -1 marks an entry that does not react; an owner's reacting entries come first in its list, and an owner has 0 to 6 of them. A value g sends the block to compute slot g % 3 of device g // 3, devices numbered with curve slowest; that device has the owner's curve index. Every value 0 to 383 appears exactly once, so each device integrates exactly 3 blocks; one owner sends at most 1 block to one device, and in every curve row some owner has 6 reacting entries and some owner has none.
All inputs are finite; a program needn't handle non-finite values.
Results may differ from the reference program's by a relative error of at most 0.0003.
Values sent between devices are 32-bit elements; how exact they have to be, the bound alone decides.
No kernel may reach another device: no remote copies, remote signals or barrier semaphores. Data moves between devices by JAX's collectives and lax.ppermute only.
A program may use at most 64 MiB of HBM per device.

```python
import math
import jax
import jax.numpy as jnp
from jax import lax

S = 53
R = 268
PARCEL_VOLUMES = 256
SUBS = 3
MAXIN = 3
BLK_DEV = 48
LIST = 6
OWNERS = 128
PARCEL_COUNT = 6144
N_GROUP = 16


def draw_burning_parcel_roster(key, part):
    owner_keys = jax.random.split(jax.random.fold_in(key, 11), OWNERS)
    chosen = jax.vmap(lambda single: jax.random.permutation(single, BLK_DEV)[:LIST])(owner_keys)
    return chosen.reshape(-1).astype(jnp.int32)


def draw_target_compute_place(key, part):
    order_key, shift_key, device_key, slot_key, owner_key = jax.random.split(jax.random.fold_in(key, 23), 5)
    row_count = OWNERS // N_GROUP
    row_number = jnp.arange(row_count, dtype=jnp.int32)
    pairing = jax.vmap(lambda number: jax.random.permutation(jax.random.fold_in(order_key, number), N_GROUP))(row_number).astype(jnp.int32)
    shifts = jax.random.randint(shift_key, (row_count, N_GROUP // 2), 0, MAXIN + 1).astype(jnp.int32)
    shifts = shifts.at[:, 0].set(MAXIN)
    counts = jnp.full((row_count, N_GROUP), MAXIN, jnp.int32)
    counts = counts.at[row_number[:, None], pairing[:, 0::2]].add(shifts)
    counts = counts.at[row_number[:, None], pairing[:, 1::2]].add(-shifts)
    owner_order = jax.vmap(lambda number: jax.random.permutation(jax.random.fold_in(owner_key, number), N_GROUP))(row_number).astype(jnp.int32)
    walked = jnp.take_along_axis(counts, owner_order, axis=1)
    passed = jnp.cumsum(walked, axis=1) - walked
    starts = jnp.zeros((row_count, N_GROUP), jnp.int32).at[row_number[:, None], owner_order].set(passed)
    position = jnp.arange(LIST, dtype=jnp.int32)
    ordinal = starts[:, :, None] + position[None, None, :]
    device_map = jax.vmap(lambda number: jax.random.permutation(jax.random.fold_in(device_key, number), N_GROUP))(row_number).astype(jnp.int32)
    local_device = jnp.take_along_axis(device_map, (ordinal % N_GROUP).reshape(row_count, -1), axis=1).reshape(row_count, N_GROUP, LIST)
    device = row_number[:, None, None] * N_GROUP + local_device
    slot_maps = jax.vmap(lambda number: jax.random.permutation(jax.random.fold_in(slot_key, number), MAXIN))(jnp.arange(OWNERS)).astype(jnp.int32)
    slot_number = slot_maps[device, jnp.minimum(ordinal // N_GROUP, MAXIN - 1)]
    reacts = position[None, None, :] < counts[:, :, None]
    return jnp.where(reacts, device * MAXIN + slot_number, -1).reshape(-1).astype(jnp.int32)


def draw_partial_reciprocal_operator(key, part):
    spread = 0.5 / math.sqrt(S)
    full_shape = (OWNERS * LIST, S, S)
    perturb = jnp.clip(jax.random.normal(key, full_shape, jnp.float32) * spread, -0.3, 0.3)
    return 0.1 * (jnp.eye(S, dtype=jnp.float32)[None] + perturb)


def with_ends(array, own_key, smallest, top_value):
    place = [jax.random.randint(jax.random.fold_in(own_key, axis), (), 0, length) for axis, length in enumerate(array.shape)]
    widest = array.shape.index(max(array.shape))
    next_to = place[:widest] + [(place[widest] + 1) % array.shape[widest]] + place[widest + 1:]
    return array.at[tuple(place)].set(smallest).at[tuple(next_to)].set(top_value)


def levels(rng, dims, pieces, low, high):
    level = 1.0
    for dim, blocks in pieces:
        draws = jax.random.uniform(jax.random.fold_in(jax.random.fold_in(rng, 6), dim), (blocks,), jnp.float32, low / len(pieces), high / len(pieces))
        level = level * jnp.repeat(jnp.exp(draws), dims[dim] // blocks).reshape((-1,) + (1,) * (len(dims) - 1 - dim))
    return level


def normal_values(stream_key, dims, scale, reach, cuts=(), held_as=jnp.bfloat16):
    values = scale * jax.random.normal(stream_key, dims, jnp.float32)
    if cuts:
        values = values * levels(stream_key, dims, cuts, -0.22, 0.18)
    return jnp.clip(values, -reach, reach).astype(held_as)


def setup_inputs(seed: int = 0) -> dict:
    streams_of = jax.random.split(jax.random.key(seed), 12)
    composition = normal_values(streams_of[0], (PARCEL_COUNT, S, PARCEL_VOLUMES), 1.0, 4.0, ((0, 128),), jnp.float32)
    heat_level = jnp.clip(1000.0 + 1500.0 * jax.random.uniform(streams_of[1], (PARCEL_COUNT, PARCEL_VOLUMES), jnp.float32) ** levels(streams_of[1], (PARCEL_COUNT, PARCEL_VOLUMES), ((0, 128),), -0.2, 0.2), 1000.0, 2500.0)
    step_counts = with_ends(jax.random.randint(streams_of[2], (PARCEL_COUNT,), 1, SUBS + 1), jax.random.fold_in(streams_of[2], 1), 1, SUBS).astype(jnp.int32)
    burning_parcel_roster = draw_burning_parcel_roster(jax.random.fold_in(streams_of[11], 71), 0)
    target_compute_place = draw_target_compute_place(jax.random.fold_in(streams_of[11], 71), 0)
    partial_reciprocal_operator = draw_partial_reciprocal_operator(jax.random.fold_in(streams_of[11], 71), 0)
    speed_log_prefactor = jnp.clip(jax.random.uniform(streams_of[6], (R,), jnp.float32, -1.0, 1.0), -1.0, 1.0)
    arrhenius_barrier = jnp.clip(jnp.exp(jax.random.uniform(streams_of[7], (R,), jnp.float32, math.log(0.5), math.log(4.0))), 0.5, 4.0)
    leading_ingredient = normal_values(streams_of[8], (R, S), S ** -0.5, 0.875, (), jnp.float32)
    trailing_ingredient = normal_values(streams_of[9], (R, S), S ** -0.5, 0.875, (), jnp.float32)
    molar_coefficients = normal_values(streams_of[10], (S, R), R ** -0.5, 0.375, (), jnp.float32)
    return {"composition": composition, "heat_level": heat_level, "step_counts": step_counts, "burning_parcel_roster": burning_parcel_roster, "target_compute_place": target_compute_place, "partial_reciprocal_operator": partial_reciprocal_operator, "speed_log_prefactor": speed_log_prefactor, "arrhenius_barrier": arrhenius_barrier, "leading_ingredient": leading_ingredient, "trailing_ingredient": trailing_ingredient, "molar_coefficients": molar_coefficients}


step_size = 0.2
section_shift = (2.0, 1.92, 0.24)
section_couple = (-8.0, 14.88, 2.4, -0.896, -0.432, -0.4)
section_weight = (19.0 / 9.0, 0.5, 25.0 / 108.0, 125.0 / 108.0)


def kinetic_speed_coefficients(heat_level, speed_log_prefactor, arrhenius_barrier):
    reciprocal_operator = 1000.0 / heat_level
    return jnp.exp(speed_log_prefactor[None, :, None] - arrhenius_barrier[None, :, None] * (reciprocal_operator[:, None, :] - 0.6))


def net_rates(present_composition, kinetic_speed_coefficient, reactants, molar_coefficients):
    paired = jnp.einsum("rs,msc->mrc", reactants, present_composition, precision=lax.Precision.HIGHEST)
    reaction_count = kinetic_speed_coefficient.shape[1]
    progress = kinetic_speed_coefficient * paired[:, :reaction_count] * paired[:, reaction_count:]
    return jnp.einsum("sr,mrc->msc", molar_coefficients, progress, precision=lax.Precision.HIGHEST)


def apply_matrix(matrix, vector):
    return jnp.einsum("mst,mtc->msc", matrix, vector, precision=lax.Precision.HIGHEST)


def advance_partial_step(present_composition, heat_level, step_counts, partial_reciprocal_operator, speed_log_prefactor, arrhenius_barrier, leading_ingredient, trailing_ingredient, molar_coefficients):
    reactants = jnp.concatenate([leading_ingredient, trailing_ingredient], axis=0)
    kinetic_speed_coefficient = kinetic_speed_coefficients(heat_level, speed_log_prefactor, arrhenius_barrier)
    weights = step_counts.astype(jnp.float32)
    per_step = (weights / step_size)[:, None, None]
    scaled = partial_reciprocal_operator / weights[:, None, None]
    for substep in range(SUBS):
        rates_one = net_rates(present_composition, kinetic_speed_coefficient, reactants, molar_coefficients)
        section_one = apply_matrix(scaled, rates_one)
        point_two = present_composition + section_shift[0] * section_one
        rates_two = net_rates(point_two, kinetic_speed_coefficient, reactants, molar_coefficients)
        section_two = apply_matrix(scaled, rates_two + section_couple[0] * per_step * section_one)
        point_three = present_composition + section_shift[1] * section_one + section_shift[2] * section_two
        rates_three = net_rates(point_three, kinetic_speed_coefficient, reactants, molar_coefficients)
        section_three = apply_matrix(scaled, rates_three + per_step * (section_couple[1] * section_one + section_couple[2] * section_two))
        section_four = apply_matrix(scaled, rates_three + per_step * (section_couple[3] * section_one + section_couple[4] * section_two + section_couple[5] * section_three))
        advanced = present_composition + section_weight[0] * section_one + section_weight[1] * section_two + section_weight[2] * section_three + section_weight[3] * section_four
        active = (substep < step_counts)[:, None, None]
        present_composition = jnp.where(active, advanced, present_composition)
    return present_composition


def reference(composition, heat_level, step_counts, burning_parcel_roster, target_compute_place, partial_reciprocal_operator, speed_log_prefactor, arrhenius_barrier, leading_ingredient, trailing_ingredient, molar_coefficients):
    entries = jnp.arange(OWNERS * LIST, dtype=jnp.int32)
    owner_of = entries // LIST
    global_block = (owner_of * BLK_DEV + burning_parcel_roster).astype(jnp.int32)
    reacts = target_compute_place >= 0
    slot_total = OWNERS * MAXIN
    target = jnp.where(reacts, target_compute_place, slot_total).astype(jnp.int32)
    sending_holder = jnp.zeros((slot_total,), jnp.int32).at[target].set(entries, mode="drop")
    slot_block = global_block[sending_holder]

    def run_device(indices):
        parcel_line_operator, item_line_operator = indices
        return advance_partial_step(composition[parcel_line_operator], heat_level[parcel_line_operator], step_counts[parcel_line_operator], partial_reciprocal_operator[item_line_operator], speed_log_prefactor, arrhenius_barrier, leading_ingredient, trailing_ingredient, molar_coefficients)

    finished = lax.map(run_device, (slot_block.reshape(OWNERS, MAXIN), sending_holder.reshape(OWNERS, MAXIN)))
    finished = finished.reshape((slot_total,) + composition.shape[1:])
    return composition.at[slot_block].set(finished)
```

```python
import functools

import jax
import jax.numpy as jnp
from jax import lax
from jax.experimental import pallas as pl
from jax.experimental.pallas import tpu as pltpu
from jax.sharding import PartitionSpec as P

SUBS = 3
STREAMS = 3

SHIFT_B1 = 1.92
SHIFT_B2 = 0.24
G1_A = (25.0 * 14.88 - 125.0 * 0.896) / 108.0
G1_AA = -(50.0 * 14.88) / 108.0
G2_A = (25.0 * 2.4 - 125.0 * 0.432) / 108.0
G2_AA = -(50.0 * 2.4) / 108.0

F32 = jnp.float32
BF16 = jnp.bfloat16


def dot(a, b):
    return jnp.dot(a, b, preferred_element_type=F32)


def halves(x):
    high = x.astype(BF16).astype(F32)
    return high, x - high


def tall(x):
    high = x.astype(BF16)
    low = (x - high.astype(F32)).astype(BF16)
    return jnp.concatenate([high, low, high], axis=0)


def wide(x):
    high, low = halves(x)
    first = high + pltpu.roll(high, 64, 1)
    return jnp.concatenate([first.astype(BF16), low.astype(BF16)], axis=1)


def after_rest(rest, x):
    rest_high, rest_low = halves(rest)
    high, low = halves(x)
    left = rest_high + pltpu.roll(rest_high, 16, 1) + pltpu.roll(rest_low, 32, 1)
    left = left + pltpu.roll(high, 64, 1)
    right = high + pltpu.roll(low, 64, 1)
    return jnp.concatenate([left.astype(BF16), right.astype(BF16)], axis=1)


def column(row, count):
    square = jnp.broadcast_to(row, (128, row.shape[1]))
    return square.T[:count]


def body(
    listed, species, reactions, cells,
    comp, heat, steps, roster, target, operator, prefactor, barrier, lead, trail, molar,
    out,
    block, heat_v, op_v, pre_v, bar_v, lead_v, trail_v, molar_v,
    steps_s, roster_s, target_s, tasks,
    y_s, kf_s, reactants_f, reactants_w, op_f, molar_f, molar_t,
    mc_s, mcrest_s, d3_s, r2_s, r3_s, e1_s,
    sems, block_sems, out_sems,
):
    copies = [
        pltpu.make_async_copy(src, dst, sems.at[i])
        for i, (src, dst) in enumerate(
            [
                (roster, roster_s),
                (steps, steps_s),
                (target, target_s),
                (operator, op_v),
                (molar, molar_v),
                (lead, lead_v),
                (trail, trail_v),
                (heat, heat_v),
                (prefactor, pre_v),
                (barrier, bar_v),
            ]
        )
    ]
    for copy in copies:
        copy.start()
    whole = pltpu.make_async_copy(comp, out, sems.at[len(copies)])

    y_s[...] = jnp.zeros_like(y_s)
    reactants_f[...] = jnp.zeros_like(reactants_f)
    op_f[...] = jnp.zeros_like(op_f)
    molar_f[...] = jnp.zeros_like(molar_f)

    for copy in copies[:3]:
        copy.wait()
    places = [roster_s[e] for e in range(listed)]
    fetches = [
        pltpu.make_async_copy(comp.at[places[e]], block.at[e], block_sems.at[e])
        for e in range(listed)
    ]
    for fetch in fetches:
        fetch.start()
    whole.start()

    counts = [steps_s[places[e]] for e in range(listed)]
    total = jnp.int32(0)
    longest = jnp.int32(0)
    for e in range(listed):
        todo = jnp.where(target_s[e] >= 0, jnp.minimum(counts[e], SUBS), 0)
        for s in range(SUBS):
            tasks[total + s] = jnp.int32(e)
        total = total + todo
        longest = jnp.maximum(longest, todo)
    length = jnp.maximum(lax.div(total + (STREAMS - 1), jnp.int32(STREAMS)), longest)
    for s in range(STREAMS * SUBS):
        tasks[total + s] = jnp.int32(listed)

    for copy in copies[3:]:
        copy.wait()

    half = reactants_f.shape[0] // 2
    reactants_f[0:reactions, 0:species] = lead_v[...]
    reactants_f[half:half + reactions, 0:species] = trail_v[...]
    molar_f[0:species, 0:reactions] = molar_v[...]
    reactants_w[...] = wide(reactants_f[...])
    molar_t[...] = tall(molar_f[...])
    lanes = molar_f.shape[1]
    pad = jnp.zeros((1, lanes - reactions), F32)
    pre_c = column(jnp.concatenate([pre_v[...].reshape(1, reactions), pad], axis=1), half)
    bar_c = column(jnp.concatenate([bar_v[...].reshape(1, reactions), pad], axis=1), half)

    rows = lax.broadcasted_iota(jnp.int32, (64, 128), 0)
    cols = lax.broadcasted_iota(jnp.int32, (64, 128), 1)
    eye = jnp.where(rows == cols, 1.0, 0.0).astype(F32)

    for e in range(listed):
        op_f[e, 0:species, 0:species] = op_v[e]
    for e in range(listed):
        m = op_f[e]
        weight = counts[e].astype(F32)
        square = dot(wide(m)[:, :192], tall(m))
        both = dot(
            jnp.concatenate([wide(m / weight), wide(square * 5.0 / weight)], axis=0)[:, :192],
            molar_t[...],
        )
        mc = both[0:64]
        d3 = (150.0 / 108.0) * mc - (50.0 / 108.0) * both[64:128]
        for store, value in ((mc_s, mc), (d3_s, d3)):
            high, low = halves(value[:, 0:256])
            store[e, 0:64] = high.astype(BF16)
            store[e, 64:128] = low.astype(BF16)
        a = 5.0 * m
        aa = 25.0 * square
        nothing = jnp.zeros((64, 128), F32)
        mcrest_s[e] = after_rest(mc[:, 256:384], nothing)[:, 0:128]
        r2_s[e] = after_rest(mc[:, 256:384], -8.0 * a)
        r3_s[e] = after_rest(d3[:, 256:384], 0.5 * eye + G2_A * a + G2_AA * aa)
        e1_s[e] = wide((19.0 / 9.0) * eye + G1_A * a + G1_AA * aa)

    for e in range(listed):
        inverse = 1000.0 / heat_v[pl.ds(places[e], 1), :] - 0.6
        for side in range(cells // 128):
            part = slice(side * 128, side * 128 + 128)
            kf_s[e, :, part] = jnp.exp(pre_c - bar_c * inverse[:, part])
    for e in range(listed):
        fetches[e].wait()
        y_s[e, 0:species] = block[e]

    def progress(stacked, e):
        paired = dot(reactants_w[:, 0:192], stacked)
        value = kf_s[e] * paired[0:half] * paired[half:2 * half]
        high = value.astype(BF16)
        low = (value - high.astype(F32)).astype(BF16)
        rest = jnp.concatenate(
            [high[256:half], low[256:half], high[256:half], jnp.zeros((16, cells), BF16)], axis=0
        )
        return high[0:256], low[0:256], rest

    def main(store, e, high, low):
        first = dot(store[e], high)
        return first[0:64] + first[64:128] + dot(store[e, 0:64], low)

    def iteration(it, carry):
        slots = [tasks[k * length + it] for k in range(STREAMS)]
        mats = [jnp.minimum(q, listed - 1) for q in slots]
        ks = range(STREAMS)
        y = [y_s[slots[k]] for k in ks]
        p = [progress(tall(y[k]), mats[k]) for k in ks]
        g1 = [main(mc_s, mats[k], p[k][0], p[k][1]) + dot(mcrest_s[mats[k], :, 0:64], p[k][2]) for k in ks]
        t1 = [tall(g1[k]) for k in ks]
        p = [progress(tall(y[k] + 2.0 * g1[k]), mats[k]) for k in ks]
        g2 = [
            main(mc_s, mats[k], p[k][0], p[k][1])
            + dot(r2_s[mats[k]], jnp.concatenate([p[k][2], t1[k]], axis=0))
            for k in ks
        ]
        y3 = [y[k] + SHIFT_B1 * g1[k] + SHIFT_B2 * g2[k] for k in ks]
        p = [progress(tall(y3[k]), mats[k]) for k in ks]
        last = [
            y[k]
            + dot(e1_s[mats[k], :, 0:192], t1[k])
            + main(d3_s, mats[k], p[k][0], p[k][1])
            + dot(r3_s[mats[k]], jnp.concatenate([p[k][2], tall(g2[k])], axis=0))
            for k in ks
        ]
        for k in ks:
            y_s[slots[k]] = last[k]
        return carry

    lax.fori_loop(0, length, iteration, jnp.int32(0))

    for e in range(listed):
        block[e] = y_s[e, 0:species]
    whole.wait()
    writes = [
        pltpu.make_async_copy(block.at[e], out.at[places[e]], out_sems.at[e])
        for e in range(listed)
    ]
    for write in writes:
        write.start()
    for write in writes:
        write.wait()


def on_device(comp, heat, steps, roster, target, operator, prefactor, barrier, lead, trail, molar):
    blocks, species, cells = comp.shape
    reactions = prefactor.shape[0]
    listed = roster.shape[0]
    half = (reactions + 15) // 16 * 16
    wide_lanes = 384
    hbm = pl.BlockSpec(memory_space=pltpu.HBM)
    kernel = functools.partial(body, listed, species, reactions, cells)
    vmem = pltpu.VMEM
    return pl.pallas_call(
        kernel,
        out_shape=jax.ShapeDtypeStruct(comp.shape, comp.dtype),
        in_specs=[hbm] * 11,
        out_specs=hbm,
        scratch_shapes=[
            vmem((listed, species, cells), F32),
            vmem(heat.shape, F32),
            vmem(operator.shape, F32),
            vmem(prefactor.shape, F32),
            vmem(barrier.shape, F32),
            vmem(lead.shape, F32),
            vmem(trail.shape, F32),
            vmem(molar.shape, F32),
            pltpu.SMEM(steps.shape, jnp.int32),
            pltpu.SMEM(roster.shape, jnp.int32),
            pltpu.SMEM(target.shape, jnp.int32),
            pltpu.SMEM((listed * SUBS + STREAMS * SUBS + 8,), jnp.int32),
            vmem((listed + 1, 64, cells), F32),
            vmem((listed, half, cells), F32),
            vmem((2 * half, 128), F32),
            vmem((2 * half, 256), BF16),
            vmem((listed, 64, 128), F32),
            vmem((64, wide_lanes), F32),
            vmem((192, wide_lanes), BF16),
            vmem((listed, 128, 256), BF16),
            vmem((listed, 64, 128), BF16),
            vmem((listed, 128, 256), BF16),
            vmem((listed, 64, 256), BF16),
            vmem((listed, 64, 256), BF16),
            vmem((listed, 64, 256), BF16),
            pltpu.SemaphoreType.DMA((11,)),
            pltpu.SemaphoreType.DMA((listed,)),
            pltpu.SemaphoreType.DMA((listed,)),
        ],
        name="integrate",
    )(comp, heat, steps, roster, target, operator, prefactor, barrier, lead, trail, molar)


def solution(mesh):
    owned = ("curve", "group")
    return jax.shard_map(
        on_device,
        mesh=mesh,
        in_specs=(
            P(owned, None, None),
            P(owned, None),
            P(owned),
            P(owned),
            P(owned),
            P(owned, None, None),
            P(),
            P(),
            P(),
            P(),
            P(),
        ),
        out_specs=P(owned, None, None),
        check_vma=False,
    )
```
